32 devices in a mesh: dp: 8 (over z, x), tensor: 4 (over y, core).
Axes of the slice: x: 2, y: 2, z: 4, core: 2. Of those that a mesh axis runs over, the one named last changes fastest.
Arguments:
- tokens: bfloat16 [24576, 1024], P(('dp', 'tensor'))
- cotangent: bfloat16 [24576, 1024], P(('dp', 'tensor')), may hold values from -6 to 6
- image_ids: int32 [24576], P('dp'), may hold values from -1 to 15, as said below
- attn_master: float32 [4, 1024, 1024], P(None, 'dp', 'tensor')
- attn_first: float32 [4, 1024, 1024], P(None, 'dp', 'tensor'), may hold values from -256 to 256
- attn_second: float32 [4, 1024, 1024], P(None, 'dp', 'tensor'), may hold values from 245.76 to 7372.8
- mlp_master: float32 [2, 1024, 4096], P(None, 'dp', 'tensor'), may hold values from -0.1875 to 0.1875
- mlp_first: float32 [2, 1024, 4096], P(None, 'dp', 'tensor'), may hold values from -256 to 256
- mlp_second: float32 [2, 1024, 4096], P(None, 'dp', 'tensor'), may hold values from 245.76 to 7372.8
- vectors: float32 [14, 1024], replicated
- vector_first: float32 [14, 1024], replicated, may hold values from -256 to 256
- vector_second: float32 [14, 1024], replicated, may hold values from 245.76 to 7372.8
Outputs:
- block_out: bfloat16 [24576, 1024], P(('dp', 'tensor'))
- grad_tokens: float32 [24576, 1024], P(('dp', 'tensor'))
- attn_grad: float32 [4, 1024, 1024], P(None, 'dp', 'tensor')
- attn_new: float32 [4, 1024, 1024], P(None, 'dp', 'tensor')
- attn_first_new: float32 [4, 1024, 1024], P(None, 'dp', 'tensor')
- attn_second_new: float32 [3, 1024, 1024], P(None, 'dp', 'tensor')
- out_second_new: float32 [1024, 1024], P('dp', 'tensor')
- attn_copy: bfloat16 [4, 1024, 1024], P(None, 'dp', 'tensor')
- mlp_grad: float32 [2, 1024, 4096], P(None, 'dp', 'tensor')
- mlp_new: float32 [2, 1024, 4096], P(None, 'dp', 'tensor')
- mlp_first_new: float32 [2, 1024, 4096], P(None, 'dp', 'tensor')
- mlp_second_new: float32 [2, 1024, 4096], P(None, 'dp', 'tensor')
- mlp_copy: bfloat16 [2, 1024, 4096], P(None, 'dp', 'tensor')
- vector_grad: float32 [14, 1024], replicated
- vector_new: float32 [14, 1024], replicated
- vector_first_new: float32 [14, 1024], replicated
- vector_second_new: float32 [14, 1024], replicated
- vector_copy: bfloat16 [14, 1024], replicated
- matrix_norms: float32 [2, 6], replicated
- row_rms: float32 [4], replicated
The draws below stay inside these ranges and needn't reach their ends.
Inputs may be any that keep to these rules, and one draw needn't show every extreme that they name: `image_ids`: every 3072 consecutive tokens hold, from their start, 1 to 2 whole images of 1370 tokens each, then padding; some group holds 2 images; every image has a number of its own.
All inputs are finite; a program needn't handle non-finite values.
Results may differ from the reference program's by a relative error of at most 0.008.
The reference program's roundings to bfloat16 on the way count: a program that leaves them out, or rounds other values in their place, can miss the bound.
Values may be sent and summed in bfloat16 or wider, within the bound.
A program may use at most 256 MiB of HBM per device.

```python
import math
import jax
import jax.numpy as jnp
from jax import lax

D = 1024
HEADS = 16
HEAD_DIM = 64
FF = 4096
IMG = 1370
IMGS = 2
STEP = 3
GROUP = 3072
TOKENS = 24576
VROWS = 14


def draw_tokens(key, part):
    row_place = jnp.arange(TOKENS).astype(jnp.float32) / (TOKENS - 1)
    noise_values = jnp.clip(jax.random.normal(key, (TOKENS, D), jnp.float32), -6.0, 6.0)
    row_scale = 1.0 + 3.0 * row_place
    return (noise_values * row_scale[:, None]).astype(jnp.bfloat16)


def draw_image_ids(key, part):
    groups = TOKENS // GROUP
    count_key, label_key = jax.random.split(key, 2)
    counts = jax.random.randint(count_key, (groups,), 1, IMGS + 1)
    labels = jax.random.permutation(label_key, groups)
    fullest = jnp.argmax(labels)
    counts = jnp.where(jnp.arange(groups) == fullest, IMGS, counts)
    slots = jnp.arange(GROUP) // IMG
    live = slots[None, :] < counts[:, None]
    numbers = labels[:, None] * IMGS + slots[None, :]
    return jnp.where(live, numbers, -1).reshape(TOKENS).astype(jnp.int32)


def draw_attn_master(key, part):
    noise_values = jax.random.normal(key, (4, D, D), jnp.float32)
    factor = jnp.where(jnp.arange(4) == 3, IMG ** 0.5, 1.0).astype(jnp.float32)
    return noise_values * factor[:, None, None] * D ** (-0.5)


def draw_vectors(key, part):
    noise_key, level_key = jax.random.split(key)
    noise_values = jax.random.normal(noise_key, (VROWS, D), jnp.float32)
    scale_level = jax.random.uniform(level_key, (VROWS, D), jnp.float32, 0.5, 1.5)
    row_index = jnp.arange(VROWS)[:, None]
    gain_rows = (row_index == 0) | (row_index == 6)
    scale_rows = (row_index == 5) | (row_index == 9)
    return jnp.where(gain_rows, 1.0 + 0.1 * noise_values, jnp.where(scale_rows, scale_level, 0.3 * noise_values))


def block_scale(own_key, extent, pieces, least, top_value):
    level = 1.0
    for dim, parts in pieces:
        steps = jax.random.uniform(jax.random.fold_in(jax.random.fold_in(own_key, 6), dim), (parts,), jnp.float32, least / len(pieces), top_value / len(pieces))
        level = level * jnp.repeat(jnp.exp(steps), extent[dim] // parts).reshape((-1,) + (1,) * (len(extent) - 1 - dim))
    return level


def normal_values(rng, dims, deviation, most, cuts=(), kind=jnp.bfloat16):
    factor_of = block_scale(rng, dims, cuts, -0.22, 0.18) if cuts else 1.0
    values = jax.random.normal(rng, dims, jnp.float32) * deviation * factor_of
    return jnp.minimum(jnp.maximum(values, -most), most).astype(kind)


def setup_inputs(seed: int = 0) -> dict:
    splits = jax.random.split(jax.random.key(seed), 13)
    tokens = draw_tokens(jax.random.fold_in(splits[12], 71), 0)
    cotangent = normal_values(splits[1], (TOKENS, D), 1.0, 6.0, ((0, 32),))
    image_ids = draw_image_ids(jax.random.fold_in(splits[12], 71), 0)
    attn_master = draw_attn_master(jax.random.fold_in(splits[12], 71), 0)
    attn_first = normal_values(splits[4], (4, D, D), (0.3 * TOKENS ** 0.5), 256.0, ((1, 8), (2, 4)), jnp.float32)
    attn_second = jnp.clip(jnp.exp(math.log(7372.8) - 3.4011974 * jax.random.uniform(splits[5], (4, D, D), jnp.float32) ** block_scale(splits[5], (4, D, D), ((1, 8), (2, 4)), -0.2, 0.2)), 245.76, 7372.8)
    mlp_master = normal_values(splits[6], (2, D, FF), D ** -0.5, 0.1875, ((1, 8), (2, 4)), jnp.float32)
    mlp_first = normal_values(splits[7], (2, D, FF), (0.3 * TOKENS ** 0.5), 256.0, ((1, 8), (2, 4)), jnp.float32)
    mlp_second = jnp.clip(jnp.exp(math.log(7372.8) - 3.4011974 * jax.random.uniform(splits[8], (2, D, FF), jnp.float32) ** block_scale(splits[8], (2, D, FF), ((1, 8), (2, 4)), -0.2, 0.2)), 245.76, 7372.8)
    vectors = draw_vectors(jax.random.fold_in(splits[12], 71), 0)
    vector_first = normal_values(splits[10], (VROWS, D), (0.3 * TOKENS ** 0.5), 256.0, (), jnp.float32)
    vector_second = jnp.clip(jnp.exp(jax.random.uniform(splits[11], (VROWS, D), jnp.float32, math.log(245.76), math.log(7372.8))), 245.76, 7372.8)
    return dict(tokens=tokens, cotangent=cotangent, image_ids=image_ids, attn_master=attn_master, attn_first=attn_first, attn_second=attn_second, mlp_master=mlp_master, mlp_first=mlp_first, mlp_second=mlp_second, vectors=vectors, vector_first=vector_first, vector_second=vector_second)


@jax.custom_vjp
def low(v):
    return lax.optimization_barrier(v.astype(jnp.bfloat16)).astype(jnp.float32)

@jax.custom_vjp
def low_back(v):
    return v

def low_keep(v):
    return (low(v), None)

def low_pass(kept, grad):
    return (grad,)

def back_keep(v):
    return (v, None)

def back_low(kept, grad):
    return (low(grad),)
low.defvjp(low_keep, low_pass)
low_back.defvjp(back_keep, back_low)
highest = lax.Precision.HIGHEST
beta_rate = 0.5
adam_epsilon = 1e-06
norm_epsilon = 1e-06
learning_rate = 0.5
vector_rate = 0.05
weight_decay = 0.05
masked_score = -1e+30

def product(left_operand, right_operand):
    return jnp.dot(left_operand, right_operand, precision=highest, preferred_element_type=jnp.float32)

def layer_norm(values, gain, shift):
    average = lax.optimization_barrier(jnp.mean(values, axis=-1, keepdims=True))
    centered = values - average
    variance = lax.optimization_barrier(jnp.mean(centered * centered, axis=-1, keepdims=True))
    return centered * lax.rsqrt(variance + norm_epsilon) * gain + shift

def group_forward(inputs, group_ids, attn_low, mlp_low, vectors):
    group_rows = inputs.shape[0]
    normed_one = low(layer_norm(inputs, vectors[0], vectors[1]))
    query = low(low_back(product(normed_one, attn_low[0]) + vectors[2]))
    key_vectors = low(low_back(product(normed_one, attn_low[1])))
    value_vectors = low(low_back(product(normed_one, attn_low[2]) + vectors[3]))
    position = jnp.arange(group_rows)
    allowed = (group_ids[:, None] == group_ids[None, :]) & (group_ids[:, None] >= 0) | (position[:, None] == position[None, :])

    def split_heads(matrix):
        return matrix.reshape(group_rows, HEADS, HEAD_DIM).transpose(1, 0, 2)

    def one_head(operands):
        head_query, head_keys, head_values = operands
        scores = low_back(product(head_query, head_keys.T) * HEAD_DIM ** (-0.5))
        scores = jnp.where(allowed, scores, masked_score)
        soft = jax.nn.softmax(scores, axis=-1)
        return product(low(soft), head_values)
    heads_out = lax.map(jax.checkpoint(one_head), (split_heads(query), split_heads(key_vectors), split_heads(value_vectors)))
    mixed = low(low_back(heads_out.transpose(1, 0, 2).reshape(group_rows, D)))
    attn_out = low_back(product(mixed, attn_low[3].T))
    branch_one = (attn_out + vectors[4]) * vectors[5]
    middle = inputs + branch_one
    normed_two = low(layer_norm(middle, vectors[6], vectors[7]))
    upper = low_back(product(normed_two, mlp_low[0]) + vectors[10:].reshape(FF))
    hidden = low(jax.nn.gelu(upper, approximate=False))
    down_output = low_back(product(hidden, mlp_low[1].T))
    branch_two = (down_output + vectors[8]) * vectors[9]
    result = middle + branch_two
    return (result, middle, branch_one, branch_two)

def adapt_moments(master, gradient, first, second):
    new_first = beta_rate * first + (1.0 - beta_rate) * gradient
    new_second = beta_rate * second + (1.0 - beta_rate) * gradient * gradient
    first_hat = new_first / (1.0 - beta_rate ** STEP)
    second_hat = new_second / (1.0 - beta_rate ** STEP)
    return (new_first, new_second, first_hat / (jnp.sqrt(second_hat) + adam_epsilon))

def reference(tokens, cotangent, image_ids, attn_master, attn_first, attn_second, mlp_master, mlp_first, mlp_second, vectors, vector_first, vector_second):
    inputs = tokens.astype(jnp.float32)
    ids_grouped = image_ids.reshape(-1, GROUP)
    valid = (image_ids >= 0).astype(jnp.float32)

    def forward(token_values, attn_weights, mlp_weights, vector_values):
        attn_low = low(attn_weights)
        mlp_low = low(mlp_weights)
        grouped = token_values.reshape(-1, GROUP, D)

        def one_group(carried, operands):
            outputs = jax.checkpoint(group_forward)(operands[0], operands[1], attn_low, mlp_low, vector_values)
            return (carried, outputs)
        unused, stacked = lax.scan(one_group, jnp.zeros((), jnp.float32), (grouped, ids_grouped))
        flat = [piece.reshape(-1, D) for piece in stacked]
        return (flat[0], (flat[0], flat[1], flat[2], flat[3]))
    result_rows, pullback, extras = jax.vjp(forward, inputs, attn_master, mlp_master, vectors, has_aux=True)
    seed_grad = cotangent.astype(jnp.float32) * valid[:, None]
    grad_tokens, attn_grad, mlp_grad, vector_grad = pullback(seed_grad)
    result, middle, branch_one, branch_two = extras
    valid_count = jnp.sum(valid)
    squares = jnp.stack([jnp.sum(valid[:, None] * field * field) for field in (middle, branch_one, result, branch_two)])
    row_rms = jnp.sqrt(squares / (valid_count * D))
    attn_first_new, attn_second_new, attn_adapted = adapt_moments(attn_master, attn_grad, attn_first, attn_second)
    mlp_first_new, mlp_second_new, mlp_adapted = adapt_moments(mlp_master, mlp_grad, mlp_first, mlp_second)
    attn_update = attn_adapted + weight_decay * attn_master
    mlp_update = mlp_adapted + weight_decay * mlp_master
    weight_norms = jnp.concatenate([jnp.sqrt(lax.optimization_barrier(jnp.sum(attn_master * attn_master, axis=(1, 2)))), jnp.sqrt(lax.optimization_barrier(jnp.sum(mlp_master * mlp_master, axis=(1, 2))))])
    update_norms = jnp.concatenate([jnp.sqrt(lax.optimization_barrier(jnp.sum(attn_update * attn_update, axis=(1, 2)))), jnp.sqrt(lax.optimization_barrier(jnp.sum(mlp_update * mlp_update, axis=(1, 2))))])
    ratios = weight_norms / update_norms
    attn_new = attn_master - learning_rate * ratios[:4, None, None] * attn_update
    mlp_new = mlp_master - learning_rate * ratios[4:, None, None] * mlp_update
    vector_first_new, vector_second_new, vector_adapted = adapt_moments(vectors, vector_grad, vector_first, vector_second)
    vector_new = vectors - vector_rate * vector_adapted
    matrix_norms = jnp.stack([weight_norms, update_norms])
    return (result_rows.astype(jnp.bfloat16), grad_tokens, attn_grad, attn_new, attn_first_new, attn_second_new[:3], attn_second_new[3], attn_new.astype(jnp.bfloat16), mlp_grad, mlp_new, mlp_first_new, mlp_second_new, mlp_new.astype(jnp.bfloat16), vector_grad, vector_new, vector_first_new, vector_second_new, vector_new.astype(jnp.bfloat16), matrix_norms, row_rms)
```

```python
import functools

import jax
import jax.numpy as jnp
from jax import lax
from jax.experimental import pallas as pl
from jax.experimental.pallas import tpu as pltpu
from jax.sharding import Mesh
from jax.sharding import PartitionSpec as P

HEAD_DIM = 64
IMAGE = 1370
STEP = 3
LANES = 128
QROWS = 352
ROW_TILE = 16
MESH = pl.DeviceIdType.MESH


beta_rate = 0.5
adam_epsilon = 1e-06
norm_epsilon = 1e-06
learning_rate = 0.5
vector_rate = 0.05
weight_decay = 0.05
masked_score = -1e30

DEVICES = ("z", "x", "y", "core")
CHIPS = ("z", "x", "y")
SWAP = ((0, 1), (1, 0))
NT = (((1,), (1,)), ((), ()))
bf16 = jnp.bfloat16
f32 = jnp.float32


def round_up(value, step):
    return -(-value // step) * step


def low_lanes():
    return lax.broadcasted_iota(jnp.int32, (QROWS, LANES), 1) < HEAD_DIM


def inside(place, limits):
    return (place < limits[0]) | ((place >= limits[1]) & (place < limits[2]))


def key_bias(limits, rows):
    place = lax.broadcasted_iota(jnp.int32, (1, rows), 1)
    return jnp.where(inside(place, limits), 0.0, masked_score)


def masked_scores(query, keys, bias):
    return lax.dot_general(query, keys, NT, preferred_element_type=f32) + bias


def attend_forward_kernel(limit_ref, q_ref, k_ref, v_ref, own_ref, out_ref, logsum_ref):
    low = low_lanes()
    query = q_ref[...] * jnp.asarray(HEAD_DIM ** (-0.5), bf16)
    keys = k_ref[...]
    values = v_ref[...]
    limits = [limit_ref[i] for i in range(3)]
    bias = key_bias(limits, keys.shape[0])
    outputs = []
    logsums = []
    for half in range(2):
        own = low if half == 0 else ~low
        scores = masked_scores(jnp.where(own, query, jnp.zeros_like(query)), keys, bias)
        largest = jnp.max(scores, axis=1, keepdims=True)
        raised = jnp.exp(scores - largest)
        totals = jnp.sum(raised, axis=1, keepdims=True)
        probs = (raised * (1.0 / totals)).astype(bf16)
        outputs.append(jnp.dot(probs, values, preferred_element_type=f32))
        logsums.append(largest + jnp.log(totals))
    row = pl.program_id(1) * QROWS + lax.broadcasted_iota(jnp.int32, (QROWS, LANES), 0)
    mixed = jnp.where(low, outputs[0], outputs[1])
    mixed = jnp.where(inside(row, limits), mixed, own_ref[...].astype(f32))
    out_ref[...] = mixed.astype(bf16)
    logsum_ref[...] = jnp.where(low, logsums[0], logsums[1])


def attend_forward(limit, query, keys, values, rows):
    pairs = query.shape[1] // LANES
    flops = 4 * 2 * pairs * rows * rows * LANES
    return pl.pallas_call(
        attend_forward_kernel,
        grid_spec=pltpu.PrefetchScalarGridSpec(
            num_scalar_prefetch=1,
            grid=(pairs, rows // QROWS),
            in_specs=[
                pl.BlockSpec((QROWS, LANES), lambda p, i, s: (i, p)),
                pl.BlockSpec((rows, LANES), lambda p, i, s: (0, p)),
                pl.BlockSpec((rows, LANES), lambda p, i, s: (0, p)),
                pl.BlockSpec((QROWS, LANES), lambda p, i, s: (i, p)),
            ],
            out_specs=[
                pl.BlockSpec((QROWS, LANES), lambda p, i, s: (i, p)),
                pl.BlockSpec((QROWS, LANES), lambda p, i, s: (i, p)),
            ],
        ),
        out_shape=(
            jax.ShapeDtypeStruct((rows, pairs * LANES), bf16),
            jax.ShapeDtypeStruct((rows, pairs * LANES), f32),
        ),
        compiler_params=pltpu.CompilerParams(vmem_limit_bytes=48 << 20),
        cost_estimate=pl.CostEstimate(
            flops=flops, bytes_accessed=8 * rows * pairs * LANES, transcendentals=2 * pairs * rows * rows
        ),
        name="attend_forward",
    )(limit, query, keys, values, values)


def attend_backward_kernel(
    limit_ref, q_ref, k_ref, v_ref, grad_ref, logsum_ref, dq_ref, dk_ref, dv_ref, keys_acc, values_acc
):
    step = pl.program_id(1)
    low = low_lanes()
    scale = jnp.asarray(HEAD_DIM ** (-0.5), bf16)
    query = q_ref[...] * scale
    keys = k_ref[...]
    values = v_ref[...]
    grads = grad_ref[...]
    bias = key_bias([limit_ref[i] for i in range(3)], keys.shape[0])

    @pl.when(step == 0)
    def _():
        keys_acc[...] = jnp.zeros_like(keys_acc)
        values_acc[...] = jnp.zeros_like(values_acc)

    outputs = []
    for half in range(2):
        own = low if half == 0 else ~low
        head_query = jnp.where(own, query, jnp.zeros_like(query))
        head_grads = jnp.where(own, grads, jnp.zeros_like(grads))
        logsum = logsum_ref[:, half * HEAD_DIM : half * HEAD_DIM + 1]
        soft = jnp.exp(masked_scores(head_query, keys, bias) - logsum)
        grad_soft = lax.dot_general(head_grads, values, NT, preferred_element_type=f32)
        inner = jnp.sum(soft * grad_soft, axis=1, keepdims=True)
        grad_scores = (soft * (grad_soft - inner)).astype(bf16)
        outputs.append(jnp.dot(grad_scores, keys, preferred_element_type=f32))
        keys_acc[...] += jnp.dot(head_query.T, grad_scores, preferred_element_type=f32)
        values_acc[...] += jnp.dot(head_grads.T, soft.astype(bf16), preferred_element_type=f32)
    dq_ref[...] = (jnp.where(low, outputs[0], outputs[1]) * HEAD_DIM ** (-0.5)).astype(bf16)

    @pl.when(step == pl.num_programs(1) - 1)
    def _():
        dk_ref[...] = keys_acc[...].astype(bf16).T
        dv_ref[...] = values_acc[...].astype(bf16).T


def attend_backward(limit, query, keys, values, grad_mixed, logsum):
    rows, columns = grad_mixed.shape
    pairs = columns // LANES
    flops = 10 * 2 * pairs * rows * rows * LANES
    shape = jax.ShapeDtypeStruct((rows, columns), bf16)
    return pl.pallas_call(
        attend_backward_kernel,
        grid_spec=pltpu.PrefetchScalarGridSpec(
            num_scalar_prefetch=1,
            grid=(pairs, rows // QROWS),
            in_specs=[
                pl.BlockSpec((QROWS, LANES), lambda p, i, s: (i, p)),
                pl.BlockSpec((rows, LANES), lambda p, i, s: (0, p)),
                pl.BlockSpec((rows, LANES), lambda p, i, s: (0, p)),
                pl.BlockSpec((QROWS, LANES), lambda p, i, s: (i, p)),
                pl.BlockSpec((QROWS, LANES), lambda p, i, s: (i, p)),
            ],
            out_specs=[
                pl.BlockSpec((QROWS, LANES), lambda p, i, s: (i, p)),
                pl.BlockSpec((rows, LANES), lambda p, i, s: (0, p)),
                pl.BlockSpec((rows, LANES), lambda p, i, s: (0, p)),
            ],
            scratch_shapes=[pltpu.VMEM((LANES, rows), f32), pltpu.VMEM((LANES, rows), f32)],
        ),
        out_shape=(shape, shape, shape),
        compiler_params=pltpu.CompilerParams(vmem_limit_bytes=48 << 20),
        cost_estimate=pl.CostEstimate(
            flops=flops, bytes_accessed=16 * rows * columns, transcendentals=2 * pairs * rows * rows
        ),
        name="attend_backward",
    )(limit, query, keys, values, grad_mixed, logsum)


def norm_parts(values):
    average = jnp.mean(values, axis=-1, keepdims=True)
    centered = values - average
    variance = jnp.mean(centered * centered, axis=-1, keepdims=True)
    inverse = lax.rsqrt(variance + norm_epsilon)
    return (centered * inverse, inverse)


def norm_back(unit, inverse, gain, grads):
    scaled = grads * gain
    first = jnp.mean(scaled, axis=-1, keepdims=True)
    second = jnp.mean(scaled * unit, axis=-1, keepdims=True)
    return inverse * (scaled - first - unit * second)


def adapt_moments(gradient, first, second):
    new_first = beta_rate * first + (1.0 - beta_rate) * gradient
    new_second = beta_rate * second + (1.0 - beta_rate) * gradient * gradient
    first_hat = new_first / (1.0 - beta_rate**STEP)
    second_hat = new_second / (1.0 - beta_rate**STEP)
    return (new_first, new_second, first_hat / (jnp.sqrt(second_hat) + adam_epsilon))


def swap_cores(values):
    return lax.ppermute(values, "core", SWAP)


def sum_cores(partial):
    sent = partial.astype(bf16)
    return sent.astype(f32) + swap_cores(sent).astype(f32)


def gather_weights(shard):
    blocks = lax.all_gather(shard, CHIPS, axis=0, tiled=False)
    outer = blocks.shape[0] // 2
    count, depth, columns = shard.shape
    blocks = blocks.reshape(outer, 2, count, depth, columns).transpose(2, 0, 3, 1, 4)
    return blocks.reshape(count, outer * depth, 2 * columns)


def scatter_grads(grads, depth, columns):
    count = grads.shape[0]
    outer = grads.shape[1] // depth
    blocks = grads.reshape(count, outer, depth, 2, columns).transpose(1, 3, 0, 2, 4)
    blocks = blocks.reshape(outer * 2, count, depth, columns)
    return lax.psum_scatter(blocks, CHIPS, scatter_dimension=0, tiled=False)


def neighbour(axis, shift):
    size = lax.axis_size(axis)
    return lax.rem(lax.axis_index(axis) + shift + size, size)


def row_plan(local_rows):
    chip_rows = 2 * local_rows
    extra = chip_rows - IMAGE
    lent = round_up(extra, ROW_TILE)
    head = round_up(IMAGE - extra, ROW_TILE)
    return (chip_rows, extra, lent, head, chip_rows + lent, round_up(head + lent, LANES))


def exchange_kernel(
    with_weights, tokens_ref, cotangent_ref, attn_ref, mlp_ref, *outs_and_scratch
):
    count = 8 if with_weights else 2
    outs = outs_and_scratch[:count]
    row_local, row_send, row_recv, own_sem, send_sem, recv_sem = outs_and_scratch[count:]
    depth = lax.axis_size("z")
    z, x, y, core = (lax.axis_index(axis) for axis in DEVICES)
    up, down = neighbour("z", 1), neighbour("z", -1)
    other_x, other_y, other_core = 1 - x, 1 - y, 1 - core

    barrier = pltpu.get_barrier_semaphore()
    greeted = [{"core": other_core}, {"y": other_y}, {"y": other_y, "core": other_core}]
    if with_weights:
        greeted += [{"z": up}, {"z": down}, {"x": other_x}]
    for device in greeted:
        pl.semaphore_signal(barrier, inc=1, device_id=device, device_id_type=MESH)
    pl.semaphore_wait(barrier, len(greeted))

    local_rows = tokens_ref.shape[0]
    chip_rows, extra, lent, head, rows, live = row_plan(local_rows)
    split = head - local_rows
    first = pl.multiple_of(core * local_rows, ROW_TILE)
    second = pl.multiple_of(core * local_rows + split + core * y * lent, ROW_TILE)
    lent_place = pl.multiple_of(y * chip_rows + (1 - y) * head, ROW_TILE)
    spans = [(0, split, first), (split, local_rows - split, second)]

    def remote(source, target, send, recv, device):
        return pltpu.make_async_remote_copy(
            src_ref=source,
            dst_ref=target,
            send_sem=send,
            recv_sem=recv,
            device_id=device,
            device_id_type=MESH,
        )

    def lend(array, source, target, to_core):
        return remote(
            source.at[pl.ds(local_rows - lent, lent)],
            target.at[pl.ds(lent_place, lent)],
            row_send.at[array, 2 + to_core],
            row_recv.at[array, 2],
            {"y": other_y, "core": to_core},
        )

    row_copies = []
    for array, source in enumerate((tokens_ref, cotangent_ref)):
        target = outs[array]
        for part, (begin, size, place) in enumerate(spans):
            window = target.at[pl.ds(place, size)]
            row_copies.append(
                (
                    pltpu.make_async_copy(
                        source.at[pl.ds(begin, size)], window, row_local.at[array, part]
                    ),
                    remote(
                        source.at[pl.ds(begin, size)],
                        window,
                        row_send.at[array, part],
                        row_recv.at[array, part],
                        {"core": other_core},
                    ),
                )
            )

    def start_rows():
        for local, shared in row_copies:
            shared.start()
            local.start()

        @pl.when(core == 1)
        def _():
            for array, source in enumerate((tokens_ref, cotangent_ref)):
                for to_core in range(2):
                    lend(array, source, outs[array], to_core).start()

    def finish_rows():
        for local, shared in row_copies:
            local.wait()
            shared.wait()
        for array, source in enumerate((tokens_ref, cotangent_ref)):
            lend(array, source, outs[array], 0).wait_recv()

        @pl.when(core == 1)
        def _():
            for array, source in enumerate((tokens_ref, cotangent_ref)):
                for to_core in range(2):
                    lend(array, source, outs[array], to_core).wait_send()

    if not with_weights:
        start_rows()
        finish_rows()
        return

    weights = []
    for index in range(6):
        source = attn_ref.at[index] if index < 4 else mlp_ref.at[index - 4]
        weights.append((index, source, outs[2 + index], source.shape[1]))

    def window(item, slot):
        index, source, target, columns = item
        return target.at[slot, x, :, pl.ds(pl.multiple_of(y * columns, LANES), columns)]

    def slot_of(step):
        return lax.rem(z - step + depth, depth)

    def local(item):
        return pltpu.make_async_copy(item[1], window(item, z), own_sem.at[item[0]])

    def ring(item, step):
        slot = slot_of(step - 1)
        source = item[1] if step == 1 else window(item, slot)
        place = step - 1
        return remote(
            source,
            window(item, slot),
            send_sem.at[item[0], place],
            recv_sem.at[item[0], place],
            {"z": up},
        )

    def by_x(item):
        return (item[0] % 2) == 0

    def cross(item, step):
        slot = slot_of(step)
        source = item[1] if step == 0 else window(item, slot)
        place = depth - 1 + step
        return remote(
            source,
            window(item, slot),
            send_sem.at[item[0], place],
            recv_sem.at[item[0], place],
            {"x": other_x} if by_x(item) else {"y": other_y},
        )

    def spread(item, step):
        index, source, target, columns = item
        slot = slot_of(step)
        if by_x(item):
            part = target.at[slot, :, :, pl.ds(pl.multiple_of(y * columns, LANES), columns)]
        else:
            part = target.at[slot, x]
        place = 2 * depth - 1 + step
        return remote(
            part,
            part,
            send_sem.at[index, place],
            recv_sem.at[index, place],
            {"y": other_y} if by_x(item) else {"x": other_x},
        )

    attn, mlp = weights[:4], weights[4:]
    for item in attn:
        ring(item, 1).start()
    for item in attn:
        cross(item, 0).start()
    for item in weights:
        local(item).start()
    start_rows()
    for item in weights:
        local(item).wait()

    def run(items, started, trailing):
        for step in range(depth):
            if step > 0:
                for item in items:
                    ring(item, step).wait_recv()
            if step + 1 < depth and (step > 0 or not started):
                for item in items:
                    ring(item, step + 1).start()
            if step == depth - 1:
                for item in trailing:
                    ring(item, 1).start()
            if step > 0 or not started:
                for item in items:
                    cross(item, step).start()
            if step > 0:
                for item in items:
                    cross(item, step - 1).wait_recv()
                    spread(item, step - 1).start()
        for item in items:
            cross(item, depth - 1).wait_recv()
            spread(item, depth - 1).start()

    def run_mlp():
        for item in mlp:
            cross(item, 0).start()
        run(mlp, True, [])

    run(attn, True, mlp)
    run_mlp()
    for item in weights:
        for step in range(depth):
            spread(item, step).wait()
            cross(item, step).wait_send()
            if step > 0:
                ring(item, step).wait_send()
    finish_rows()


def exchange(tokens, cotangent, attn_low, mlp_low, with_weights):
    local_rows, width = tokens.shape
    rows = row_plan(local_rows)[4]
    depth = lax.axis_size("z")
    shapes = [jax.ShapeDtypeStruct((rows, width), bf16)] * 2
    if with_weights:
        for weights in (attn_low, mlp_low):
            count, block, columns = weights.shape
            shapes += [jax.ShapeDtypeStruct((depth, 2, block, 2 * columns), bf16)] * count
    vmem = pl.BlockSpec(memory_space=pltpu.VMEM)
    places = 3 * depth - 1 if with_weights else 1
    outs = pl.pallas_call(
        functools.partial(exchange_kernel, with_weights),
        in_specs=[vmem] * 4,
        out_specs=[pl.BlockSpec(memory_space=pl.ANY)] * len(shapes),
        out_shape=shapes,
        scratch_shapes=[
            pltpu.SemaphoreType.DMA((2, 2)),
            pltpu.SemaphoreType.DMA((2, 4)),
            pltpu.SemaphoreType.DMA((2, 3)),
            pltpu.SemaphoreType.DMA((6,)),
            pltpu.SemaphoreType.DMA((6, places)),
            pltpu.SemaphoreType.DMA((6, places)),
        ],
        compiler_params=pltpu.CompilerParams(collective_id=0, has_side_effects=True),
        name="exchange",
    )(tokens, cotangent, attn_low, mlp_low)
    if with_weights:
        weights = [w.reshape(-1, w.shape[-1]) for w in outs[2:]]
    else:
        weights = list(gather_weights(attn_low)) + list(gather_weights(mlp_low))
    return (outs[0], outs[1], weights)


def scatter_short(grads, columns, by_x):
    depth = lax.axis_size("z")
    z, x, y, _ = (lax.axis_index(axis) for axis in DEVICES)
    block = grads.shape[0] // (2 * depth)

    def trade_y(values):
        sent = lax.dynamic_slice_in_dim(values, (1 - y) * columns, columns, values.ndim - 1)
        kept = lax.dynamic_slice_in_dim(values, y * columns, columns, values.ndim - 1)
        return kept.astype(f32) + lax.ppermute(sent.astype(bf16), "y", SWAP).astype(f32)

    def trade_x(values):
        sent = lax.dynamic_index_in_dim(values, 1 - x, 1, False)
        kept = lax.dynamic_index_in_dim(values, x, 1, False)
        return kept.astype(f32) + lax.ppermute(sent.astype(bf16), "x", SWAP).astype(f32)

    blocks = grads.reshape(depth, 2, block, 2 * columns)
    blocks = trade_y(trade_x(blocks)) if by_x else trade_x(trade_y(blocks))
    ring = tuple((i, (i + 1) % depth) for i in range(depth))
    moving = lax.dynamic_index_in_dim(blocks, lax.rem(z - 1 + depth, depth), 0, False)
    for step in range(1, depth):
        moving = lax.ppermute(moving.astype(bf16), "z", ring).astype(f32)
        place = lax.rem(z - 1 - step + 2 * depth, depth)
        moving = moving + lax.dynamic_index_in_dim(blocks, place, 0, False)
    return moving


def scatter_all(grads, depth, columns):
    if lax.axis_size("z") > 4:
        return scatter_grads(jnp.stack(grads), depth, columns)
    return jnp.stack([scatter_short(g, columns, i % 2 == 0) for i, g in enumerate(grads)])


def per_device(
    tokens,
    cotangent,
    image_ids,
    attn_master,
    attn_first,
    attn_second,
    mlp_master,
    mlp_first,
    mlp_second,
    vectors,
    vector_first,
    vector_second,
):
    local_rows, width = tokens.shape
    chip_rows, extra, lent, head, rows, live = row_plan(local_rows)
    core = lax.axis_index("core")
    upper_chip = lax.axis_index("y") == 1
    first_core = (core == 0).astype(f32)
    head_part = attn_master.shape[2]
    hidden_part = mlp_master.shape[2]

    attn_low = attn_master.astype(bf16)
    mlp_low = mlp_master.astype(bf16)
    arranged, seeds, weights = exchange(
        tokens, cotangent, attn_low, mlp_low, lax.axis_size("z") <= 4
    )
    query_full, key_full, value_full, out_full, up_full, down_full = weights

    image_live = lax.dynamic_slice(image_ids, (jnp.where(upper_chip, IMAGE, 0),), (1,)) >= 0
    whole = jnp.array([IMAGE, 0, 0], jnp.int32)
    parted = jnp.array([IMAGE - extra, head + lent - extra, head + lent], jnp.int32)
    limit = jnp.where(image_live, jnp.where(upper_chip, parted, whole), 0)
    valid = inside(jnp.arange(live), limit).astype(f32)[:, None]

    inputs = arranged.astype(f32)
    unit_one, inverse_one = norm_parts(inputs)
    normed_one = (unit_one * vectors[0] + vectors[1]).astype(bf16)

    def own_columns(row, part):
        return lax.dynamic_index_in_dim(row.reshape(2, 2, part), core, 1, False).reshape(-1)

    query_bias = own_columns(vectors[2], head_part)
    value_bias = own_columns(vectors[3], head_part)
    up_bias = own_columns(vectors[10:].reshape(-1), hidden_part)

    def project(matrix, bias):
        product = jnp.dot(normed_one, matrix, preferred_element_type=f32)
        return (product if bias is None else product + bias).astype(bf16)

    query = project(query_full, query_bias)
    keys = project(key_full, None)
    values = project(value_full, value_bias)
    attended, logsum = attend_forward(limit, query, keys, values, live)
    mixed = jnp.concatenate([attended, values[live:]], 0)
    attn_out = sum_cores(lax.dot_general(mixed, out_full, NT, preferred_element_type=f32))
    shifted_out = attn_out + vectors[4]
    branch_one = shifted_out * vectors[5]
    middle = inputs + branch_one
    unit_two, inverse_two = norm_parts(middle)
    normed_two = (unit_two * vectors[6] + vectors[7]).astype(bf16)

    upper = jnp.dot(normed_two, up_full, preferred_element_type=f32) + up_bias
    spread = 0.5 * (1.0 + lax.erf(upper * 0.5**0.5))
    hidden = (upper * spread).astype(bf16)
    slope = spread + upper * jnp.exp(-0.5 * upper * upper) * 0.3989422804014327
    down = sum_cores(lax.dot_general(hidden, down_full, NT, preferred_element_type=f32))
    shifted_down = down + vectors[8]
    branch_two = shifted_down * vectors[9]
    result = middle + branch_two

    seed = seeds[:live].astype(f32) * valid
    scaled_seed = seed * vectors[9]
    grad_down = scaled_seed.astype(bf16)
    live_hidden = hidden[:live]
    grad_down_weight = jnp.einsum("gd,gf->df", grad_down, live_hidden, preferred_element_type=f32)
    grad_hidden = jnp.dot(grad_down, down_full, preferred_element_type=f32)
    grad_upper = (grad_hidden * slope[:live]).astype(bf16)
    grad_up_weight = jnp.einsum(
        "gd,gf->df", normed_two[:live], grad_upper, preferred_element_type=f32
    )
    grad_normed_two = sum_cores(
        lax.dot_general(grad_upper, up_full, NT, preferred_element_type=f32)
    )
    grad_middle = seed + norm_back(
        unit_two[:live], inverse_two[:live], vectors[6], grad_normed_two
    )
    scaled_middle = grad_middle * vectors[5]
    grad_attn_out = scaled_middle.astype(bf16)
    grad_out_weight = jnp.einsum(
        "gd,gk->dk", grad_attn_out, mixed[:live], preferred_element_type=f32
    )
    grad_mixed = jnp.dot(grad_attn_out, out_full, preferred_element_type=f32).astype(bf16)
    grad_heads = attend_backward(limit, query, keys, values, grad_mixed, logsum)
    live_one = normed_one[:live]
    grad_attn = [
        jnp.einsum("gd,gk->dk", live_one, g, preferred_element_type=f32) for g in grad_heads
    ] + [grad_out_weight]
    grad_normed_one = sum_cores(
        sum(
            lax.dot_general(g, w, NT, preferred_element_type=f32)
            for g, w in zip(grad_heads, weights)
        )
    )
    grad_tokens = grad_middle + norm_back(
        unit_one[:live], inverse_one[:live], vectors[0], grad_normed_one
    )

    def own_rows(values):
        place = head + lent
        back = lax.ppermute(values[head:place], "y", ((1, 0),))
        seam = chip_rows - lent
        mine = jnp.arange(seam, chip_rows)[:, None] < IMAGE
        lower = jnp.concatenate(
            [values[local_rows:seam], jnp.where(mine, pad_rows(values)[seam:chip_rows], back)], 0
        )
        upper = jnp.concatenate([values[local_rows:head], pad_rows(values)[place:rows]], 0)
        return jnp.where(core == 0, values[:local_rows], jnp.where(upper_chip, upper, lower))

    def pad_rows(values):
        missing = jnp.zeros((rows - values.shape[0], width), values.dtype)
        return jnp.concatenate([values, missing], 0)

    block_out = own_rows(result.astype(bf16))
    grad_tokens_own = own_rows(grad_tokens)

    def square_sum(values):
        return jnp.sum(valid * values[:live] * values[:live])

    stat_terms = first_core * jnp.stack(
        [
            jnp.sum(valid),
            square_sum(middle),
            square_sum(branch_one),
            square_sum(result),
            square_sum(branch_two),
        ]
    )
    weight_local_sq = jnp.concatenate(
        [
            jnp.sum(attn_master * attn_master, axis=(1, 2)),
            jnp.sum(mlp_master * mlp_master, axis=(1, 2)),
        ]
    )

    def placed(values, part):
        zero = jnp.zeros((2, 2, part), f32)
        return lax.dynamic_update_index_in_dim(
            zero, values.reshape(2, part), core, 1
        ).reshape(-1, width)

    def column_sum(values):
        return jnp.sum(values.astype(f32), axis=0)

    shared_rows = first_core * jnp.stack(
        [
            column_sum(grad_normed_one * unit_one[:live]),
            column_sum(grad_normed_one),
            column_sum(scaled_middle),
            column_sum(grad_middle * shifted_out[:live]),
            column_sum(grad_normed_two * unit_two[:live]),
            column_sum(grad_normed_two),
            column_sum(scaled_seed),
            column_sum(seed * shifted_down[:live]),
        ]
    )
    vector_local = jnp.concatenate(
        [
            shared_rows[:2],
            placed(column_sum(grad_heads[0]), head_part),
            placed(column_sum(grad_heads[2]), head_part),
            shared_rows[2:],
            placed(column_sum(grad_upper), hidden_part),
        ],
        axis=0,
    )
    vector_total = lax.psum(vector_local, DEVICES)
    row_totals = lax.psum(stat_terms, DEVICES)
    mlp_shard = scatter_all(
        [grad_up_weight, grad_down_weight], mlp_master.shape[1], hidden_part
    )
    attn_shard = scatter_all(grad_attn, attn_master.shape[1], head_part)

    attn_first_new, attn_second_new, attn_adapted = adapt_moments(
        attn_shard, attn_first, attn_second
    )
    mlp_first_new, mlp_second_new, mlp_adapted = adapt_moments(mlp_shard, mlp_first, mlp_second)
    attn_update = attn_adapted + weight_decay * attn_master
    mlp_update = mlp_adapted + weight_decay * mlp_master
    update_local_sq = jnp.concatenate(
        [
            jnp.sum(attn_update * attn_update, axis=(1, 2)),
            jnp.sum(mlp_update * mlp_update, axis=(1, 2)),
        ]
    )
    weight_sq, update_sq = lax.psum((weight_local_sq, update_local_sq), DEVICES)
    weight_norms = jnp.sqrt(weight_sq)
    update_norms = jnp.sqrt(update_sq)
    ratios = weight_norms / update_norms
    attn_new = attn_master - learning_rate * ratios[:4, None, None] * attn_update
    mlp_new = mlp_master - learning_rate * ratios[4:, None, None] * mlp_update
    vector_first_new, vector_second_new, vector_adapted = adapt_moments(
        vector_total, vector_first, vector_second
    )
    vector_new = vectors - vector_rate * vector_adapted
    matrix_norms = jnp.stack([weight_norms, update_norms])
    row_rms = jnp.sqrt(row_totals[1:] / (row_totals[0] * width))
    return (
        block_out,
        grad_tokens_own,
        attn_shard,
        attn_new,
        attn_first_new,
        attn_second_new[:3],
        attn_second_new[3],
        attn_new.astype(bf16),
        mlp_shard,
        mlp_new,
        mlp_first_new,
        mlp_second_new,
        mlp_new.astype(bf16),
        vector_total,
        vector_new,
        vector_first_new,
        vector_second_new,
        vector_new.astype(bf16),
        matrix_norms,
        row_rms,
    )


def solution(mesh):
    outer = mesh.shape["dp"]
    chips = Mesh(mesh.devices.reshape(outer // 2, 2, 2, 2), DEVICES)
    dp = ("z", "x")
    tensor = ("y", "core")
    row_spec = P(dp + tensor, None)
    weight_spec = P(None, dp, tensor)
    in_specs = (row_spec, row_spec, P(dp)) + (weight_spec,) * 6 + (P(),) * 3
    out_specs = (
        (row_spec, row_spec)
        + (weight_spec,) * 4
        + (P(dp, tensor),)
        + (weight_spec,) * 6
        + (P(),) * 7
    )
    return jax.shard_map(
        per_device, mesh=chips, in_specs=in_specs, out_specs=out_specs, check_vma=False
    )
```
